128 devices in a mesh: dp: 8 (over x, z_hi), tp: 16 (over z_lo, y, core).
Axes of the slice: x: 4, y: 4, z: 4 (z_hi: 2, z_lo: 2; z = z_hi * 2 + z_lo), core: 2. Of those that a mesh axis runs over, the one named last changes fastest.
Arguments:
- hidden_in: bfloat16 [4, 64, 4096], P(None, 'dp'), may hold values from -6 to 6
- pre_gain: float32 [4096], replicated, may hold values from 0.25 to 1.75
- w_zx: bfloat16 [4096, 2, 8192], P(None, None, 'tp'), may hold values from -0.09375 to 0.09375
- zx_codes: bfloat16 [4096, 2, 8192], P(('dp', 'tp')), may hold values from -4 to 4
- zx_exponents: int32 [32, 2, 64], P('dp', None, 'tp'), may hold values from -9 to -6
- w_bc: bfloat16 [4096, 2048], P(None, 'tp'), may hold values from -0.09375 to 0.09375
- w_dt: bfloat16 [4096, 128], P(None, 'tp'), may hold values from -0.09375 to 0.09375
- conv_x: float32 [5, 8192], P(None, 'tp'), may hold values from -0.6 to 0.6
- conv_bc: float32 [5, 2048], P(None, 'tp'), may hold values from -0.6 to 0.6
- dt_bias: float32 [128], P('tp'), may hold values from -2 to 0.5
- decay_rate: float32 [128], P('tp'), may hold values from 0.05 to 2
- skip_gain: float32 [128], P('tp'), may hold values from 0.5 to 1.5
- conv_state_x: bfloat16 [64, 3, 8192], P('dp', None, 'tp'), may hold values from -6 to 6
- conv_state_bc: bfloat16 [64, 3, 2048], P('dp', None, 'tp'), may hold values from -6 to 6
- ssm_state: float32 [64, 128, 64, 256], P('dp', 'tp'), may hold values from -6 to 6
- norm_gain: float32 [8192], P('tp'), may hold values from 0.25 to 1.75
- w_out: bfloat16 [8192, 4096], P('tp'), may hold values from -0.0625 to 0.0625
- out_codes: bfloat16 [8192, 4096], P('tp', 'dp'), may hold values from -4 to 4
- out_exponents: int32 [64, 32], P('tp', 'dp'), may hold values from -7 to -4
Outputs:
- mixed: bfloat16 [4, 64, 4096], P(None, 'dp', 'tp')
- final_state: float32 [64, 128, 64, 256], P('dp', 'tp')
The draws below stay inside these ranges and needn't reach their ends.
All inputs are finite; a program needn't handle non-finite values.
Results may differ from the reference program's by a relative error of at most 0.014.
Values may be sent and summed in bfloat16 or wider, within the bound.
No kernel may reach another device: no remote copies, remote signals or barrier semaphores. Data moves between devices by JAX's collectives and lax.ppermute only.
A program may use at most 128 MiB of HBM per device.

```python
import math
import jax
import jax.numpy as jnp
from jax import lax

D = 4096
H = 128
P_SIZE = 64
N = 256
G = 4
BLK = 128
STEPS = 4
DI = 8192
ROWS = 64


def set_ends(drawn, own_key, smallest, top_value):
    longest = drawn.shape.index(max(drawn.shape))
    spots = []
    for shift in (0, 1):
        where = [jax.random.randint(jax.random.fold_in(own_key, axis), (), 0, length) for axis, length in enumerate(drawn.shape)]
        where[longest] = (where[longest] + shift) % drawn.shape[longest]
        spots.append(tuple(where))
    return drawn.at[spots[0]].set(smallest).at[spots[1]].set(top_value)


def block_scale(rng, dims, shards, smallest, top_value):
    loudness, own = 1.0, jax.random.fold_in(rng, 6)
    for dim, blocks in shards:
        draws = jnp.exp(jax.random.uniform(jax.random.fold_in(own, dim), (blocks,), jnp.float32, smallest / len(shards), top_value / len(shards)))
        loudness = loudness * jnp.repeat(draws, dims[dim] // blocks).reshape([-1 if axis == dim else 1 for axis in range(len(dims))])
    return loudness


def bell_draw(own_key, dims, width, bound, split=(), held_as=jnp.bfloat16):
    gain = block_scale(own_key, dims, split, -0.22, 0.18) if split else 1.0
    array = jax.random.normal(own_key, dims, jnp.float32) * width * gain
    return jnp.minimum(jnp.maximum(array, -bound), bound).astype(held_as)


def setup_inputs(seed: int = 0) -> dict:
    seeds = jax.random.split(jax.random.key(seed), 20)
    return {
        "hidden_in": bell_draw(seeds[0], (STEPS, ROWS, D), 1.0, 6.0, ((1, 8),)),
        "pre_gain": jnp.clip(1.0 + 0.15 * jax.random.normal(seeds[1], (D,), jnp.float32), 0.25, 1.75),
        "w_zx": bell_draw(seeds[2], (D, 2, DI), D ** -0.5, 0.09375, ((2, 16),)),
        "zx_codes": bell_draw(seeds[3], (D, 2, DI), 1.0, 4.0, ((0, 128),)),
        "zx_exponents": set_ends(jax.random.randint(seeds[4], (D // BLK, 2, DI // BLK), -9, -5), jax.random.fold_in(seeds[4], 1), -9, (-5) - 1).astype(jnp.int32),
        "w_bc": bell_draw(seeds[5], (D, 2 * G * N), D ** -0.5, 0.09375, ((1, 16),)),
        "w_dt": bell_draw(seeds[6], (D, H), D ** -0.5, 0.09375, ((1, 16),)),
        "conv_x": jnp.clip(jax.random.uniform(seeds[7], (5, DI), jnp.float32, -0.6, 0.6) * block_scale(seeds[7], (5, DI), ((1, 16),), -0.4, 0.0), -0.6, 0.6),
        "conv_bc": jnp.clip(jax.random.uniform(seeds[8], (5, 2 * G * N), jnp.float32, -0.6, 0.6) * block_scale(seeds[8], (5, 2 * G * N), ((1, 16),), -0.4, 0.0), -0.6, 0.6),
        "dt_bias": jnp.clip(-2.0 + 2.5 * jax.random.uniform(seeds[9], (H,), jnp.float32) ** block_scale(seeds[9], (H,), ((0, 16),), -0.2, 0.2), -2.0, 0.5),
        "decay_rate": jnp.clip(jnp.exp(math.log(2.0) - 3.6888794 * jax.random.uniform(seeds[10], (H,), jnp.float32) ** block_scale(seeds[10], (H,), ((0, 16),), -0.2, 0.2)), 0.05, 2.0),
        "skip_gain": jnp.clip(0.5 + 1.0 * jax.random.uniform(seeds[11], (H,), jnp.float32) ** block_scale(seeds[11], (H,), ((0, 16),), -0.2, 0.2), 0.5, 1.5),
        "conv_state_x": bell_draw(seeds[12], (ROWS, 3, DI), 1.0, 6.0, ((0, 8), (2, 16))),
        "conv_state_bc": bell_draw(seeds[13], (ROWS, 3, 2 * G * N), 1.0, 6.0, ((0, 8), (2, 16))),
        "ssm_state": bell_draw(seeds[14], (ROWS, H, P_SIZE, N), 1.0, 6.0, ((0, 8), (1, 16)), jnp.float32),
        "norm_gain": jnp.clip(1.0 + 0.15 * jax.random.normal(seeds[15], (DI,), jnp.float32), 0.25, 1.75),
        "w_out": bell_draw(seeds[16], (DI, D), DI ** -0.5, 0.0625, ((0, 16),)),
        "out_codes": bell_draw(seeds[17], (DI, D), 1.0, 4.0, ((0, 16), (1, 8))),
        "out_exponents": set_ends(jax.random.randint(seeds[18], (DI // BLK, D // BLK), -7, -3), jax.random.fold_in(seeds[18], 1), -7, (-3) - 1).astype(jnp.int32),
    }


EPS = 1e-05

def decode_pairs(codes, exponents, block):
    rows, pair, cols = codes.shape
    blocked = codes.astype(jnp.float32).reshape(rows // block, block, pair, cols // block, block)
    scales = jnp.exp2(exponents.astype(jnp.float32))
    return (blocked * scales[:, None, :, :, None]).reshape(rows, pair, cols)

def decode_matrix(codes, exponents, block):
    rows, cols = codes.shape
    blocked = codes.astype(jnp.float32).reshape(rows // block, block, cols // block, block)
    scales = jnp.exp2(exponents.astype(jnp.float32))
    return (blocked * scales[:, None, :, None]).reshape(rows, cols)

def conv_step(history, fresh, params):
    window = jnp.concatenate([history, fresh[:, None, :]], axis=1)
    mixed = lax.optimization_barrier(jnp.sum(window * params[:4][None], axis=1)) + params[4]
    return (jax.nn.silu(mixed), window[:, 1:])

def reference(hidden_in, pre_gain, w_zx, zx_codes, zx_exponents, w_bc, w_dt, conv_x, conv_bc, dt_bias, decay_rate, skip_gain, conv_state_x, conv_state_bc, ssm_state, norm_gain, w_out, out_codes, out_exponents):
    new_zx = (w_zx.astype(jnp.float32) + decode_pairs(zx_codes, zx_exponents, BLK)).astype(jnp.bfloat16)
    new_out = (w_out.astype(jnp.float32) + decode_matrix(out_codes, out_exponents, BLK)).astype(jnp.bfloat16)
    zx_flat = new_zx.reshape(D, 2 * DI)
    history_x = conv_state_x.astype(jnp.float32)
    history_bc = conv_state_bc.astype(jnp.float32)
    state = ssm_state
    results = []
    for step in range(STEPS):
        x = hidden_in[step].astype(jnp.float32)
        if step > 0:
            x = x + results[-1].astype(jnp.float32)
        rows = x.shape[0]
        normed = (x * lax.rsqrt(lax.optimization_barrier(jnp.mean(x * x, -1, keepdims=True)) + EPS) * pre_gain).astype(jnp.bfloat16)
        zx = jnp.dot(normed, zx_flat, preferred_element_type=jnp.float32).reshape(rows, 2, DI)
        gate = zx[:, 0]
        inner = zx[:, 1]
        bc_raw = jnp.dot(normed, w_bc, preferred_element_type=jnp.float32)
        dt_raw = jnp.dot(normed, w_dt, preferred_element_type=jnp.float32)
        conv_inner, history_x = conv_step(history_x, inner, conv_x)
        conv_state_out, history_bc = conv_step(history_bc, bc_raw, conv_bc)
        b_heads = jnp.repeat(conv_state_out[:, :G * N].reshape(rows, G, N), H // G, axis=1)
        c_heads = jnp.repeat(conv_state_out[:, G * N:].reshape(rows, G, N), H // G, axis=1)
        step_size = jax.nn.softplus(dt_raw + dt_bias)
        decay = jnp.exp(-step_size * decay_rate)
        inner_heads = conv_inner.reshape(rows, H, P_SIZE)
        state = decay[:, :, None, None] * state + (step_size[:, :, None] * inner_heads)[:, :, :, None] * b_heads[:, :, None, :]
        read = jnp.einsum('rhpn,rhn->rhp', state, c_heads, precision=lax.Precision.HIGHEST) + skip_gain[:, None] * inner_heads
        gated = (read.reshape(rows, DI) * jax.nn.silu(gate)).reshape(rows, G, DI // G)
        grouped = gated * lax.rsqrt(lax.optimization_barrier(jnp.mean(gated * gated, -1, keepdims=True)) + EPS)
        scaled = (grouped.reshape(rows, DI) * norm_gain).astype(jnp.bfloat16)
        results.append(jnp.dot(scaled, new_out, preferred_element_type=jnp.float32).astype(jnp.bfloat16))
    return (jnp.stack(results), state)
```

```python
import functools

import jax
import jax.numpy as jnp
from jax import lax
from jax.experimental import pallas as pl
from jax.experimental.pallas import tpu as pltpu
from jax.sharding import PartitionSpec as P

H = 128
G = 4
BLK = 128
STEPS = 4
DI = 8192
D = 4096
EPS = 1e-05
DP = 8
TP = 16
ROWS = 64
R = 8
F = D // DP
C = DI // TP
N = 256
HEADS = H // TP
PS = 64
PEERS = TP // G
NZ = 2 * C + 2 * N + 128
NQ = C + 128
SLAB = F + 48

BF = jnp.bfloat16
F32 = jnp.float32
VM = pl.BlockSpec(memory_space=pltpu.VMEM)
SM = pl.BlockSpec(memory_space=pltpu.SMEM)
PARAMS = pltpu.CompilerParams(vmem_limit_bytes=20 * 2**20)


def split_pair(value):
    high = value.astype(BF).astype(F32)
    return high, value - high


def lanes(rows):
    return lax.broadcasted_iota(jnp.int32, (rows, 128), 1)


def project(x, gain_ref, w_ref, out_ref):
    v = (x * gain_ref[...]).astype(BF)
    squares = jnp.sum(x * x, axis=-1, keepdims=True)
    zx = jnp.dot(v, w_ref[...], preferred_element_type=F32)
    high, low = split_pair(squares)
    spot = lanes(ROWS)
    last = zx[:, NZ - 128 :]
    last = jnp.where(spot == HEADS, high, jnp.where(spot == HEADS + 1, low, last))
    out_ref[:, : NZ - 128] = zx[:, : NZ - 128].astype(BF)
    out_ref[:, NZ - 128 : NZ] = last.astype(BF)


def first_kernel(hid_ref, gain_ref, w_ref, out_ref):
    project(hid_ref[...].astype(F32), gain_ref, w_ref, out_ref)


def group_sum(parts_ref, first, rows):
    total = jnp.zeros((rows, parts_ref.shape[2] - 128), F32)
    for g in range(G):
        part = jnp.zeros_like(total)
        pair = jnp.zeros((rows, 128), F32)
        for k in range(PEERS):
            slab = parts_ref[first + g * PEERS + k].astype(F32)
            part = part + slab[:, :-128]
            pair = pair + slab[:, -128:]
        squares = pair[:, 0:1] + pair[:, 1:2]
        total = total + part * lax.rsqrt(squares / (DI // G) + EPS)
    return total


def next_kernel(parts_ref, hid_ref, gain_ref, w_ref, out_ref):
    mixed = group_sum(parts_ref, 0, ROWS).astype(BF)
    out_ref[:, NZ:] = mixed
    project(hid_ref[...].astype(F32) + mixed.astype(F32), gain_ref, w_ref, out_ref)


def silu(value):
    return value / (1.0 + jnp.exp(-value))


def state_kernel(
    has_mixed,
    where_ref,
    zx_ref,
    hx0_ref,
    hx1_ref,
    hx2_ref,
    hb0_ref,
    hb1_ref,
    hb2_ref,
    cx_ref,
    cb_ref,
    head_ref,
    gain_ref,
    state_ref,
    out_ref,
    inner_ref,
    bc_ref,
    new_ref,
    *rest,
):
    if has_mixed:
        mixed_ref, xt_ref, dt_ref, rd_ref = rest
    else:
        xt_ref, dt_ref, rd_ref = rest
    z = zx_ref[0][:, :NZ].astype(F32)
    for k in range(1, DP):
        z = z + zx_ref[k][:, :NZ].astype(F32)
    tail = z[:, NZ - 128 :]
    squares = tail[:, HEADS : HEADS + 1] + tail[:, HEADS + 1 : HEADS + 2]
    z = z * lax.rsqrt(squares / D + EPS)
    gate = z[:, :C]
    inner = z[:, C : 2 * C]
    bc = z[:, 2 * C : 2 * C + 2 * N]
    inner_ref[...] = inner
    bc_ref[...] = bc
    conv_x = silu(
        hx0_ref[...] * cx_ref[0:1]
        + hx1_ref[...] * cx_ref[1:2]
        + hx2_ref[...] * cx_ref[2:3]
        + inner * cx_ref[3:4]
        + cx_ref[4:5]
    )
    conv_bc = silu(
        hb0_ref[...] * cb_ref[0:1]
        + hb1_ref[...] * cb_ref[1:2]
        + hb2_ref[...] * cb_ref[2:3]
        + bc * cb_ref[3:4]
        + cb_ref[4:5]
    )
    spot = lanes(R)
    raw = jnp.concatenate(
        [
            jnp.where(
                spot < PS,
                z[:, NZ - 128 + 2 * j : NZ - 128 + 2 * j + 1],
                z[:, NZ - 128 + 2 * j + 1 : NZ - 128 + 2 * j + 2],
            )
            for j in range(HEADS // 2)
        ],
        axis=1,
    )
    raw = raw + head_ref[0:1]
    step_size = jnp.maximum(raw, 0.0) + jnp.log1p(jnp.exp(-jnp.abs(raw)))
    decay = jnp.exp(-step_size * head_ref[1:2])
    xt_ref[:, :R] = (step_size * conv_x).T
    dt_ref[:, :R] = decay.T

    def one_head(h, carry):
        span = pl.ds(pl.multiple_of(h * PS, PS), PS)
        for r in range(R):
            fresh = dt_ref[span, r : r + 1] * state_ref[r, h] + xt_ref[span, r : r + 1] * conv_bc[r : r + 1, :N]
            new_ref[r, h] = fresh
            rd_ref[span, r : r + 1] = jnp.sum(fresh * conv_bc[r : r + 1, N:], axis=-1, keepdims=True)
        return carry

    lax.fori_loop(0, HEADS, one_head, 0)
    read = rd_ref[:, :R].T + head_ref[2:3] * conv_x
    gated = read * silu(gate)
    high, low = split_pair(jnp.sum(gated * gated, axis=-1, keepdims=True))
    message = (gated * gain_ref[...]).astype(BF)
    pair = jnp.where(spot == 0, high, jnp.where(spot == 1, low, 0.0)).astype(BF)
    for k in range(DP):
        out_ref[k, :, :C] = message
        out_ref[k, :, C:] = pair
    if has_mixed:
        slot = where_ref[1]
        half = pl.multiple_of(NZ + lax.rem(slot, 2) * 256, 128)
        mixed_ref[...] = zx_ref[slot // 2, :, pl.ds(half, 256)]


def out_kernel(q_ref, w_ref, out_ref):
    part = jnp.dot(q_ref[:, :C], w_ref[...], preferred_element_type=F32).astype(BF)
    pair = q_ref[:, C:]
    for k in range(TP):
        out_ref[k, :, :C] = part
        out_ref[k, :, C:] = pair


def last_kernel(where_ref, q_ref, w_ref, out_ref):
    part = jnp.dot(q_ref[:, :C], w_ref[...], preferred_element_type=F32).astype(BF)
    pair = q_ref[:, C:]
    out_ref[...] = jnp.zeros_like(out_ref)
    me = where_ref[0]
    for k in range(DP):
        for half in range(2):
            slot = k * TP + 2 * me + half
            out_ref[slot, :, :256] = part[k * R : k * R + R, half * 256 : half * 256 + 256]
            out_ref[slot, :, 256:] = pair[k * R : k * R + R]


def finish_kernel(where_ref, parts_ref, out_ref):
    out_ref[...] = group_sum(parts_ref, (where_ref[1] // 2) * TP, R).astype(BF)


def struct(shape, dtype):
    return jax.ShapeDtypeStruct(shape, dtype)


def call(kernel, outs, operands, **extra):
    return pl.pallas_call(
        kernel,
        out_shape=outs,
        in_specs=[SM if o.dtype == jnp.int32 else VM for o in operands],
        out_specs=jax.tree.map(lambda _: VM, outs),
        compiler_params=PARAMS,
        **extra,
    )(*operands)


def swap(value, axis):
    return lax.all_to_all(value, axis, 0, 0, tiled=True)


def decode_pairs(codes, exponents, block):
    rows, pair, cols = codes.shape
    blocked = codes.astype(jnp.float32).reshape(rows // block, block, pair, cols // block, block)
    scales = jnp.exp2(exponents.astype(jnp.float32))
    return (blocked * scales[:, None, :, :, None]).reshape(rows, pair, cols)


def decode_matrix(codes, exponents, block):
    rows, cols = codes.shape
    blocked = codes.astype(jnp.float32).reshape(rows // block, block, cols // block, block)
    scales = jnp.exp2(exponents.astype(jnp.float32))
    return (blocked * scales[:, None, :, None]).reshape(rows, cols)


def group_parameters(w_bc_rows, conv_bc, conv_state_bc, slot):
    high = conv_bc.astype(BF)
    rest = conv_bc - high.astype(F32)
    mid = rest.astype(BF)
    low = (rest - mid.astype(F32)).astype(BF)
    history = jnp.moveaxis(conv_state_bc, 1, 0).reshape(3 * R, 128)
    slab = jnp.concatenate([w_bc_rows, history, high, mid, low, jnp.zeros((SLAB - F - 39, 128), BF)], 0)
    needed = [[2 * g, 2 * g + 1, 8 + 2 * g, 9 + 2 * g] for g in range(G)]
    got = []
    for turn in range(PEERS):
        pairs = [(needed[g][(i + turn) % PEERS], g * PEERS + i) for g in range(G) for i in range(PEERS)]
        got.append(lax.ppermute(slab, "tp", pairs))
    first = (PEERS - slot % PEERS) % PEERS
    wide = jnp.stack(got + got)
    mine = lax.dynamic_slice_in_dim(wide, first, PEERS, 0)
    whole = jnp.moveaxis(mine, 0, 1).reshape(SLAB, 2 * N)
    taps = whole[F + 24 : F + 39].astype(F32)
    return whole[:F], whole[F : F + 24].astype(F32), taps[0:5] + taps[5:10] + taps[10:15]


def body(
    hidden_in,
    pre_gain,
    w_zx,
    zx_codes,
    zx_exponents,
    w_bc,
    w_dt,
    conv_x,
    conv_bc,
    dt_bias,
    decay_rate,
    skip_gain,
    conv_state_x,
    conv_state_bc,
    ssm_state,
    norm_gain,
    w_out,
    out_codes,
    out_exponents,
):
    replica = lax.axis_index("dp")
    slot = lax.axis_index("tp")
    where = jnp.stack([replica, slot]).astype(jnp.int32)

    traded = lax.all_to_all(zx_codes, "tp", split_axis=2, concat_axis=0, tiled=True)
    hid = swap(jnp.moveaxis(hidden_in.reshape(STEPS, R, DP, F), 2, 0), "dp")
    hid = jnp.moveaxis(hid, 1, 0).reshape(STEPS, ROWS, F)
    w_bc_rows = lax.dynamic_slice_in_dim(w_bc, replica * F, F, 0)
    bc_weights, history_bc, taps_bc = group_parameters(w_bc_rows, conv_bc, conv_state_bc, slot)

    w_rows = lax.dynamic_slice_in_dim(w_zx, replica * F, F, 0)
    zx_weights = (
        (w_rows.astype(F32) + decode_pairs(traded, zx_exponents, BLK)).astype(BF).reshape(F, 2 * C)
    )
    dt_rows = jnp.pad(lax.dynamic_slice_in_dim(w_dt, replica * F, F, 0), ((0, 0), (0, 128 - HEADS)))
    weights = jnp.concatenate([zx_weights, bc_weights, dt_rows], 1)
    w_out_cols = lax.dynamic_slice_in_dim(w_out, replica * 512, 512, 1)
    out_weights = (w_out_cols.astype(F32) + decode_matrix(out_codes, out_exponents, BLK)).astype(BF)

    gain = lax.dynamic_slice_in_dim(pre_gain, replica * F, F, 0)[None]
    head = jnp.repeat(jnp.stack([dt_bias, decay_rate, skip_gain]), PS, axis=1)
    norm = norm_gain[None]
    hx = [conv_state_x[:, k].astype(F32) for k in range(3)]
    hb = [history_bc[k * R : k * R + R] for k in range(3)]
    state = ssm_state
    results = []
    parts = None
    for step in range(STEPS):
        if step == 0:
            zx = call(first_kernel, struct((ROWS, NZ), BF), [hid[0], gain, weights])
        else:
            zx = call(next_kernel, struct((ROWS, NZ + 512), BF), [parts, hid[step], gain, weights])
        zx = swap(zx.reshape(DP, R, -1), "dp")
        outs = [
            struct((DP, R, NQ), BF),
            struct((R, C), F32),
            struct((R, 2 * N), F32),
            struct(state.shape, F32),
        ]
        if step > 0:
            outs.append(struct((R, 256), BF))
        got = call(
            functools.partial(state_kernel, step > 0),
            outs,
            [where, zx, *hx, *hb, conv_x, taps_bc, head, norm, state],
            scratch_shapes=[pltpu.VMEM((C, 128), F32)] * 3,
            input_output_aliases={12: 3} if step else {},
        )
        q, inner, bc, state = got[:4]
        if step > 0:
            results.append(got[4])
        hx = hx[1:] + [inner]
        hb = hb[1:] + [bc]
        q = swap(q, "dp").reshape(ROWS, NQ)
        if step + 1 < STEPS:
            parts = swap(call(out_kernel, struct((TP, ROWS, NQ), BF), [q, out_weights]), "tp")
        else:
            tiles = call(last_kernel, struct((DP * TP, R, 384), BF), [where, q, out_weights])
            tiles = lax.all_to_all(tiles, ("dp", "tp"), 0, 0, tiled=True)
            results.append(call(finish_kernel, struct((R, 256), BF), [where, tiles]))
    return (jnp.stack(results), state)


def solution(mesh):
    return jax.shard_map(
        body,
        mesh=mesh,
        in_specs=(
            P(None, "dp", None),
            P(),
            P(None, None, "tp"),
            P(("dp", "tp"), None, None),
            P("dp", None, "tp"),
            P(None, "tp"),
            P(None, "tp"),
            P(None, "tp"),
            P(None, "tp"),
            P("tp"),
            P("tp"),
            P("tp"),
            P("dp", None, "tp"),
            P("dp", None, "tp"),
            P("dp", "tp", None, None),
            P("tp"),
            P("tp", None),
            P("tp", "dp"),
            P("tp", "dp"),
        ),
        out_specs=(P(None, "dp", "tp"), P("dp", "tp", None, None)),
        check_vma=False,
    )
```

```python
import functools

import jax
import jax.numpy as jnp
from jax import lax
from jax.experimental import pallas as pl
from jax.experimental.pallas import tpu as pltpu
from jax.sharding import PartitionSpec as P

H = 128
G = 4
BLK = 128
STEPS = 4
DI = 8192
D = 4096
EPS = 1e-05
DP = 8
TP = 16
ROWS = 64
R = 8
F = D // DP
C = DI // TP
N = 256
HEADS = H // TP
PS = 64
PEERS = TP // G
NZ = 2 * C + 2 * N + 128
NQ = C + 128
SLAB = F + 48

BF = jnp.bfloat16
F32 = jnp.float32
VM = pl.BlockSpec(memory_space=pltpu.VMEM)
HB = pl.BlockSpec(memory_space=pltpu.HBM)
SM = pl.BlockSpec(memory_space=pltpu.SMEM)
PARAMS = pltpu.CompilerParams(vmem_limit_bytes=20 * 2**20)
WHOLE = pltpu.CompilerParams(vmem_limit_bytes=60 * 1024 * 2**10)


def split_pair(value):
    high = value.astype(BF).astype(F32)
    return high, value - high


def lanes(rows):
    return lax.broadcasted_iota(jnp.int32, (rows, 128), 1)


def product(left, right_ref):
    return jnp.dot(left, right_ref[...], preferred_element_type=F32)


def project(x, gain_ref, wz_ref, wbc_ref, wdt_ref, out_ref):
    v = (x * gain_ref[...]).astype(BF)
    high, low = split_pair(jnp.sum(x * x, axis=-1, keepdims=True))
    spot = lanes(ROWS)
    last = product(v, wdt_ref)
    last = jnp.where(spot == HEADS, high, jnp.where(spot == HEADS + 1, low, last))
    out_ref[:, : 2 * C] = product(v, wz_ref).astype(BF)
    out_ref[:, 2 * C : NZ - 128] = product(v, wbc_ref).astype(BF)
    out_ref[:, NZ - 128 : NZ] = last.astype(BF)


def fresh_rows(hid_ref, step):
    return hid_ref[:, step].astype(F32).reshape(ROWS, F)


def first_kernel(hid_ref, *refs):
    project(fresh_rows(hid_ref, 0), *refs)


def pack_kernel(codes_ref, out_ref):
    for k in range(TP):
        out_ref[k] = jnp.transpose(codes_ref[:, :, k * C : k * C + C], (1, 0, 2))


def decode_kernel(codes_ref, w_ref, scale_ref, out_ref):
    depth = F // TP
    for k in range(BLK // depth):
        for pair in range(2):
            row = pl.program_id(0) * 2 + pair
            delta = codes_ref[k, pair].astype(F32) * scale_ref[pl.ds(row, 1)]
            old = w_ref[pair, k * depth : k * depth + depth].astype(F32)
            out_ref[k * depth : k * depth + depth, pair * C : pair * C + C] = (old + delta).astype(BF)


def slab_kernel(where_ref, w_hbm, taps_ref, history_ref, out_ref, w_ref, sem):
    first = pl.multiple_of(where_ref[0] * F, F)
    copy = pltpu.make_async_copy(w_hbm.at[pl.ds(first, F)], w_ref, sem.at[0])
    copy.start()
    out_ref[F : F + 24] = history_ref[...].astype(F32).reshape(24, 128).astype(BF)
    rest = jnp.concatenate([taps_ref[...], jnp.zeros((3, 128), F32)], axis=0)
    for k in range(3):
        piece = rest.astype(BF)
        out_ref[F + 24 + 8 * k : F + 32 + 8 * k] = piece
        rest = rest - piece.astype(F32)
    copy.wait()
    out_ref[:F] = w_ref[...]


def wide_heads(row):
    spot = lanes(1)
    return jnp.concatenate(
        [jnp.where(spot < PS, row[:, 2 * j : 2 * j + 1], row[:, 2 * j + 1 : 2 * j + 2]) for j in range(HEADS // 2)],
        axis=1,
    )


def setup_kernel(where_ref, *refs):
    got = refs[:PEERS]
    conv_ref, bias_ref, rate_ref, skip_ref, norm_ref, history_ref, w_ref, past_ref = refs[PEERS:]
    place = lax.rem(where_ref[1], PEERS)
    for k in range(PEERS):
        mine = got[k][...].astype(F32)
        for i in range(1, PEERS):
            mine = jnp.where(place == i, got[(k - i) % PEERS][...].astype(F32), mine)
        span = slice(k * 128, k * 128 + 128)
        w_ref[:, span] = mine[:F].astype(BF)
        for j in range(3):
            past_ref[3 + j, :, span] = mine[F + R * j : F + R * j + R]
        taps = mine[F + 24 : F + 32] + mine[F + 32 : F + 40] + mine[F + 40 : F + 48]
        past_ref[6, 5:8, span] = taps[:3]
        past_ref[7, 0:2, span] = taps[3:5]
    for j in range(3):
        past_ref[j] = history_ref[j].astype(F32)
    past_ref[6, 0:5] = conv_ref[...]
    past_ref[7, 2:3] = wide_heads(bias_ref[...])
    past_ref[7, 3:4] = wide_heads(rate_ref[...])
    past_ref[7, 4:5] = wide_heads(skip_ref[...])
    past_ref[7, 5:6] = norm_ref[...]
    past_ref[7, 6:8] = jnp.zeros((2, C), F32)


def group_sum(parts_ref, first):
    pairs = []
    for g in range(G):
        pair = parts_ref[first + g * PEERS, -R:, :128].astype(F32)
        for k in range(1, PEERS):
            pair = pair + parts_ref[first + g * PEERS + k, -R:, :128].astype(F32)
        pairs.append(lax.rsqrt((pair[0:1] + pair[1:2]) / (DI // G) + EPS))
    scales = jnp.concatenate(pairs + pairs, axis=0).T
    rows = parts_ref.shape[1] - R
    total = jnp.zeros((rows, 256), F32)
    for g in range(G):
        part = parts_ref[first + g * PEERS, :rows].astype(F32)
        for k in range(1, PEERS):
            part = part + parts_ref[first + g * PEERS + k, :rows].astype(F32)
        total = total + part * scales[:rows, g : g + 1]
    return total


def half_kernel(parts_ref, out_ref):
    out_ref[...] = group_sum(parts_ref, 0).astype(BF)


def next_kernel(step, where_ref, mine_ref, other_ref, hid_ref, *refs):
    even = lax.rem(where_ref[1], 2) == 0
    mine, other = mine_ref[...].astype(F32), other_ref[...].astype(F32)
    mixed = jnp.concatenate([jnp.where(even, mine, other), jnp.where(even, other, mine)], axis=1)
    refs[-1][:, NZ:] = mixed.astype(BF)
    project(fresh_rows(hid_ref, step) + mixed, *refs)


def silu(value):
    return value / (1.0 + jnp.exp(-value))


def across(left, right):
    return lax.dot_general(left, right, (((1,), (1,)), ((), ())), preferred_element_type=F32)


def convolve(past_ref, first, fresh, params, tap):
    total = fresh * params[tap + 3 : tap + 4] + params[tap + 4 : tap + 5]
    for k in range(3):
        total = total + past_ref[first + k] * params[tap + k : tap + k + 1]
    return silu(total)


def read_kernel(
    has_mixed,
    where_ref,
    zx_hbm,
    past_hbm,
    state_hbm,
    out_ref,
    kept_ref,
    change_ref,
    *rest,
):
    zx_ref, past_ref, state_ref, small_sems, row_sems = rest[-5:]
    arrive = pltpu.make_async_copy(zx_hbm, zx_ref, small_sems.at[0])
    small = pltpu.make_async_copy(past_hbm, past_ref, small_sems.at[1])
    arrive.start()
    small.start()
    large = [pltpu.make_async_copy(state_hbm.at[r], state_ref.at[r], row_sems.at[r]) for r in range(R)]
    for copy in large:
        copy.start()
    arrive.wait()
    z = zx_ref[0][:, :NZ].astype(F32)
    for k in range(1, DP):
        z = z + zx_ref[k][:, :NZ].astype(F32)
    tail = z[:, NZ - 128 :]
    squares = tail[:, HEADS : HEADS + 1] + tail[:, HEADS + 1 : HEADS + 2]
    z = z * lax.rsqrt(squares / D + EPS)
    gate = z[:, :C]
    inner = z[:, C : 2 * C]
    bc = z[:, 2 * C : 2 * C + 2 * N]
    small.wait()
    params = past_ref[6:].reshape(2 * R, C)
    conv_x = convolve(past_ref, 0, inner, params, 0)
    conv_bc = convolve(past_ref, 3, bc, params, 5)
    for k in range(2):
        kept_ref[k] = past_ref[k + 1]
        kept_ref[3 + k] = past_ref[4 + k]
    kept_ref[2] = inner
    kept_ref[5] = bc
    kept_ref[6:] = past_ref[6:]
    head = params[10:13]
    gain = params[13:14]
    spot = lanes(R)
    columns = [z[:, NZ - 128 + k : NZ - 127 + k] for k in range(HEADS)]
    raw = jnp.concatenate([jnp.where(spot < PS, *columns[2 * j : 2 * j + 2]) for j in range(HEADS // 2)], axis=1)
    raw = raw + head[0:1]
    step_size = jnp.maximum(raw, 0.0) + jnp.log1p(jnp.exp(-jnp.abs(raw)))
    decay = jnp.exp(-step_size * head[1:2])
    added = step_size * conv_x
    change_ref[0] = decay
    change_ref[1] = added
    change_ref[2] = conv_bc
    b, c = conv_bc[:, :N], conv_bc[:, N:]
    high, low = split_pair(c)
    probe = jnp.concatenate([high, low], axis=0).astype(BF)
    row = lax.broadcasted_iota(jnp.int32, (R, C), 0)
    sums = jnp.zeros((R, C), F32)
    for r in range(R):
        large[r].wait()
        old = state_ref[r]
        high = old.astype(BF)
        low = (old - high.astype(F32)).astype(BF)
        total = across(probe, high) + across(probe, low)
        sums = jnp.where(row == r, total[:R] + total[R:], sums)
    read = decay * sums + added * jnp.sum(b * c, axis=-1, keepdims=True) + head[2:3] * conv_x
    gated = read * silu(gate)
    high, low = split_pair(jnp.sum(gated * gated, axis=-1, keepdims=True))
    message = (gated * gain).astype(BF)
    pair = jnp.where(spot == 0, high, jnp.where(spot == 1, low, 0.0)).astype(BF)
    for k in range(DP):
        out_ref[k, :, :C] = message
        out_ref[k, :, C:] = pair
    if has_mixed:
        mixed_ref = rest[0]
        slot = where_ref[1]
        half = pl.multiple_of(NZ + lax.rem(slot, 2) * 256, 128)
        mixed_ref[...] = zx_ref[slot // 2, :, pl.ds(half, 256)]


def update_kernel(change_ref, state_ref, new_ref, left_ref):
    r = pl.program_id(0)

    @pl.when(r == 0)
    def _():
        high, low = split_pair(change_ref[1])
        left_ref[...] = jnp.concatenate([high, low, high], axis=0).T.astype(BF)

    high, low = split_pair(change_ref[2, :, :N])
    right = jnp.concatenate([high, high, low], axis=0)
    row = lax.rem(lax.broadcasted_iota(jnp.int32, (3 * R, N), 0), R)
    outer = jnp.dot(left_ref[...], jnp.where(row == r, right, 0.0).astype(BF), preferred_element_type=F32)
    decay = change_ref[0, pl.ds(r, 1)]
    for k in range(HEADS):
        span = slice(k * PS, k * PS + PS)
        new_ref[0, span] = decay[:, k * PS : k * PS + 1] * state_ref[0, span] + outer[span]


def out_parts(q_ref, w_ref):
    part = jnp.dot(q_ref[:, :C], w_ref[...], preferred_element_type=F32).astype(BF)
    pair = q_ref[:, C:].astype(F32)
    pair = jnp.concatenate([pair, jnp.zeros_like(pair)], axis=0).T[:R]
    return part, pair


def out_kernel(q_ref, w_ref, out_ref):
    part, pair = out_parts(q_ref, w_ref)
    pair = jnp.concatenate([pair, pair], axis=1).astype(BF)
    for k in range(TP):
        half = (k % 2) * 256
        out_ref[k, :ROWS] = part[:, half : half + 256]
        out_ref[k, ROWS:] = pair


def last_kernel(where_ref, q_ref, w_ref, out_ref):
    part, pair = out_parts(q_ref, w_ref)
    out_ref[...] = jnp.zeros_like(out_ref)
    me = where_ref[0]
    for k in range(DP):
        mine = jnp.concatenate([pair[:, k * R : k * R + R], jnp.zeros((R, 256 - R), F32)], axis=1).astype(BF)
        for half in range(2):
            slot = k * TP + 2 * me + half
            out_ref[slot, :R] = part[k * R : k * R + R, half * 256 : half * 256 + 256]
            out_ref[slot, R:] = mine


def finish_kernel(where_ref, parts_ref, out_ref):
    out_ref[...] = group_sum(parts_ref, (where_ref[1] // 2) * TP).astype(BF)


def struct(shape, dtype):
    return jax.ShapeDtypeStruct(shape, dtype)


def call(kernel, outs, operands, remote=0, compiler_params=PARAMS, **extra):
    near = operands[: len(operands) - remote]
    return pl.pallas_call(
        kernel,
        out_shape=outs,
        in_specs=[SM if o.dtype == jnp.int32 else VM for o in near] + [HB] * remote,
        out_specs=jax.tree.map(lambda _: VM, outs),
        compiler_params=compiler_params,
        **extra,
    )(*operands)


def swap(value, axis):
    return lax.all_to_all(value, axis, 0, 0, tiled=True)


def decode_matrix(codes, exponents, block):
    rows, cols = codes.shape
    blocked = codes.astype(jnp.float32).reshape(rows // block, block, cols // block, block)
    scales = jnp.exp2(exponents.astype(jnp.float32))
    return (blocked * scales[:, None, :, None]).reshape(rows, cols)


def group_slabs(slab):
    needed = [[2 * g, 2 * g + 1, 8 + 2 * g, 9 + 2 * g] for g in range(G)]
    got = []
    for turn in range(PEERS):
        pairs = [(needed[g][(i + turn) % PEERS], g * PEERS + i) for g in range(G) for i in range(PEERS)]
        got.append(lax.ppermute(slab, "tp", pairs))
    return got


def body(
    hidden_in,
    pre_gain,
    w_zx,
    zx_codes,
    zx_exponents,
    w_bc,
    w_dt,
    conv_x,
    conv_bc,
    dt_bias,
    decay_rate,
    skip_gain,
    conv_state_x,
    conv_state_bc,
    ssm_state,
    norm_gain,
    w_out,
    out_codes,
    out_exponents,
):
    replica = lax.axis_index("dp")
    slot = lax.axis_index("tp")
    where = jnp.stack([replica, slot]).astype(jnp.int32)

    packed = call(pack_kernel, struct((TP, 2, F // TP, C), BF), [zx_codes])
    split = jnp.moveaxis(hidden_in.reshape(STEPS, R, DP, F), 2, 0)
    split, w_bc = lax.optimization_barrier((split, w_bc))
    hid = swap(split, "dp")
    slab = pl.pallas_call(
        slab_kernel,
        out_shape=struct((SLAB, 128), BF),
        in_specs=[SM, HB, VM, VM],
        out_specs=VM,
        scratch_shapes=[pltpu.VMEM((F, 128), BF), pltpu.SemaphoreType.DMA((1,))],
        compiler_params=WHOLE,
    )(where, w_bc, conv_bc, jnp.moveaxis(conv_state_bc, 1, 0))
    got = group_slabs(slab)
    packed, hid = lax.optimization_barrier((packed, hid))
    traded = swap(packed, "tp")
    bc_weights, past = call(
        setup_kernel,
        [struct((F, 2 * N), BF), struct((8, R, C), F32)],
        [
            where,
            *got,
            conv_x,
            dt_bias[None],
            decay_rate[None],
            skip_gain[None],
            norm_gain[None],
            jnp.moveaxis(conv_state_x, 1, 0),
        ],
    )

    w_rows = jnp.transpose(lax.dynamic_slice_in_dim(w_zx, replica * F, F, 0), (1, 0, 2))
    scales = jnp.repeat(jnp.exp2(zx_exponents.astype(F32)), BLK, axis=2).reshape(8, C)
    zx_weights = pl.pallas_call(
        decode_kernel,
        out_shape=struct((F, 2 * C), BF),
        grid=(F // BLK,),
        in_specs=[
            pl.BlockSpec((TP * BLK // F, 2, F // TP, C), lambda k: (k, 0, 0, 0)),
            pl.BlockSpec((2, BLK, C), lambda k: (0, k, 0)),
            pl.BlockSpec((8, C), lambda k: (0, 0)),
        ],
        out_specs=pl.BlockSpec((BLK, 2 * C), lambda k: (k, 0)),
        compiler_params=WHOLE,
    )(traded, w_rows, scales)
    dt_weights = jnp.pad(lax.dynamic_slice_in_dim(w_dt, replica * F, F, 0), ((0, 0), (0, 128 - HEADS)))
    w_out_cols = lax.dynamic_slice_in_dim(w_out, replica * 512, 512, 1)
    out_weights = (w_out_cols.astype(F32) + decode_matrix(out_codes, out_exponents, BLK)).astype(BF)

    gain = lax.dynamic_slice_in_dim(pre_gain, replica * F, F, 0)[None]
    state = ssm_state.reshape(R, C, N)
    fixed = [gain, zx_weights, bc_weights, dt_weights]
    results = []
    mine = other = None
    for step in range(STEPS):
        if step == 0:
            zx = call(first_kernel, struct((ROWS, NZ), BF), [hid, *fixed])
        else:
            zx = call(
                functools.partial(next_kernel, step),
                struct((ROWS, NZ + 512), BF),
                [where, mine, other, hid, *fixed],
            )
        zx = swap(zx.reshape(DP, R, -1), "dp")
        outs = [
            struct((DP, R, NQ), BF),
            struct(past.shape, F32),
            struct((3, R, C), F32),
        ]
        if step > 0:
            outs.append(struct((R, 256), BF))
        q, past, change, *mixed = call(
            functools.partial(read_kernel, step > 0),
            outs,
            [where, zx, past, state],
            remote=3,
            compiler_params=WHOLE,
            scratch_shapes=[
                pltpu.VMEM(zx.shape, BF),
                pltpu.VMEM(past.shape, F32),
                pltpu.VMEM(state.shape, F32),
                pltpu.SemaphoreType.DMA((2,)),
                pltpu.SemaphoreType.DMA((R,)),
            ],
        )
        results += mixed
        block = pl.BlockSpec((1, C, N), lambda r: (r, 0, 0))
        state = pl.pallas_call(
            update_kernel,
            out_shape=struct(state.shape, F32),
            grid=(R,),
            in_specs=[pl.BlockSpec((3, R, C), lambda r: (0, 0, 0)), block],
            out_specs=block,
            scratch_shapes=[pltpu.VMEM((C, 3 * R), BF)],
            compiler_params=WHOLE,
            cost_estimate=pl.CostEstimate(flops=4 * 10**9, transcendentals=0, bytes_accessed=8 * 2**20),
        )(change, state)
        q = swap(q, "dp").reshape(ROWS, NQ)
        if step + 1 < STEPS:
            parts = swap(call(out_kernel, struct((TP, ROWS + R, 256), BF), [q, out_weights]), "tp")
            mine = call(half_kernel, struct((ROWS, 256), BF), [parts])
            other = lax.ppermute(mine, "tp", [(k, k ^ 1) for k in range(TP)])
        else:
            tiles = call(last_kernel, struct((DP * TP, 2 * R, 256), BF), [where, q, out_weights])
            tiles = lax.all_to_all(tiles, ("dp", "tp"), 0, 0, tiled=True)
            results.append(call(finish_kernel, struct((R, 256), BF), [where, tiles]))
    return (jnp.stack(results), state.reshape(ssm_state.shape))


def solution(mesh):
    return jax.shard_map(
        body,
        mesh=mesh,
        in_specs=(
            P(None, "dp", None),
            P(),
            P(None, None, "tp"),
            P(("dp", "tp"), None, None),
            P("dp", None, "tp"),
            P(None, "tp"),
            P(None, "tp"),
            P(None, "tp"),
            P(None, "tp"),
            P("tp"),
            P("tp"),
            P("tp"),
            P("dp", None, "tp"),
            P("dp", None, "tp"),
            P("dp", "tp", None, None),
            P("tp"),
            P("tp", None),
            P("tp", "dp"),
            P("tp", "dp"),
        ),
        out_specs=(P(None, "dp", "tp"), P("dp", "tp", None, None)),
        check_vma=False,
    )
```
